32 devices in a mesh: gx: 4 (over x, core), gy: 4 (over z), gz: 2 (over y).
Axes of the slice: x: 2, y: 2, z: 4, core: 2. Of those that a mesh axis runs over, the one named last changes fastest.
Arguments:
- columns: int32 [1024, 2048], P(('gx', 'gy', 'gz')), may hold values from 0 to 32767, as said below
- counts: int32 [1024, 2048], P(('gx', 'gy', 'gz')), may hold values from 1 to 63
- nnz_count: int32 [1024], P(('gx', 'gy', 'gz')), may hold values from 1 to 2048, as said below
- selected: int32 [2048], replicated, may hold values from 0 to 32767, as said below
Outputs:
- gene_stats: float32 [2, 32768], P(None, 'gz')
- pca_input: bfloat16 [1024, 2048], P(('gx', 'gy'), 'gz')
The draws below stay inside these ranges and needn't reach their ends.
Inputs may be any that keep to these rules, and one draw needn't show every extreme that they name: `columns`: in each row no two slots fall in the same block of 16 consecutive genes (so the first nnz_count slots hold distinct genes); slots beyond nnz_count are not part of the matrix. For every k, the live slots of one cell fall on at most 128 of the genes selected[k * 2048 / 2] to selected[(k + 1) * 2048 / 2 - 1]; some cell reaches 128 for every k in every draw. `nnz_count`: some cell has all 2048 slots live in every draw. `selected`: distinct genes.
All inputs are finite; a program needn't handle non-finite values.
Results may differ from the reference program's by a relative error of at most 0.0085.
Values may be sent and summed in bfloat16 or wider, within the bound.
A program may use at most 128 MiB of HBM per device.

```python
import jax
import jax.numpy as jnp
from jax import lax

GENES = 32768
SEL = 2048
NNZ_MAX = 2048
CELLS = 1024
N_GZ = 2


def block_plan(key):
    stride = GENES // NNZ_MAX
    share_size = SEL // N_GZ
    per_owner = 2 * share_size // stride
    block_order = jax.random.permutation(jax.random.fold_in(key, 31), jnp.arange(NNZ_MAX, dtype=jnp.int32))[:N_GZ * per_owner]
    block_order = block_order.reshape(N_GZ, per_owner).astype(jnp.int32)
    block_keys = jax.random.split(jax.random.fold_in(key, 32), N_GZ * per_owner)
    lane_perm = jax.vmap(lambda one_key: jax.random.permutation(one_key, jnp.arange(stride, dtype=jnp.int32)))(block_keys)
    return (block_order, lane_perm.reshape(N_GZ, per_owner, stride).astype(jnp.int32))


def full_cell(key):
    return jax.random.randint(jax.random.fold_in(key, 41), (), 0, CELLS, dtype=jnp.int32)


def draw_columns(key, part):
    stride = GENES // NNZ_MAX
    block_order, lane_perm = block_plan(key)
    forced = jnp.full((NNZ_MAX,), -1, jnp.int32).at[block_order.reshape(-1)].set(lane_perm[:, :, 0].reshape(-1))
    jitter = jax.random.randint(jax.random.fold_in(key, 12), (CELLS, NNZ_MAX), 0, stride, dtype=jnp.int32)
    cell_ids = lax.broadcasted_iota(jnp.int32, (CELLS, NNZ_MAX), 0)
    pinned = (cell_ids == full_cell(key)) & (forced[None, :] >= 0)
    jitter = jnp.where(pinned, forced[None, :], jitter)
    block_ids = lax.broadcasted_iota(jnp.int32, (CELLS, NNZ_MAX), 1)
    genes_drawn = block_ids * stride + jitter
    shuffled = jax.random.permutation(jax.random.fold_in(key, 14), genes_drawn, axis=1, independent=True)
    return shuffled.astype(jnp.int32)


def draw_nnz_count(key, part):
    cell_ids = jnp.arange(CELLS, dtype=jnp.int32)
    lowest = NNZ_MAX // 3
    base = lowest + (NNZ_MAX - lowest) * cell_ids // max(CELLS - 1, 1)
    floor_count = jnp.maximum(base // 2, 1)
    spread = base - floor_count + 1
    draw_bits = jax.random.randint(jax.random.fold_in(key, 21), (CELLS,), 0, 1 << 20, dtype=jnp.int32)
    picked = floor_count + draw_bits * spread // (1 << 20)
    picked = jnp.where(cell_ids == full_cell(key), NNZ_MAX, picked)
    return jnp.clip(picked, 1, NNZ_MAX).astype(jnp.int32)


def draw_selected(key, part):
    stride = GENES // NNZ_MAX
    share_size = SEL // N_GZ
    per_owner = 2 * share_size // stride
    block_order, lane_perm = block_plan(key)
    gene_grid = block_order[:, :, None] * stride + lane_perm
    anchors = gene_grid[:, :, 0]
    others = gene_grid[:, :, 1:].reshape(N_GZ, per_owner * (stride - 1))
    other_keys = jax.random.split(jax.random.fold_in(key, 33), N_GZ)
    others = jax.vmap(lambda one_key, row_genes: jax.random.permutation(one_key, row_genes))(other_keys, others)
    others = others[:, :share_size - per_owner]
    chosen = jnp.concatenate([anchors, others], axis=1)
    order_keys = jax.random.split(jax.random.fold_in(key, 34), N_GZ)
    chosen = jax.vmap(lambda one_key, row_genes: jax.random.permutation(one_key, row_genes))(order_keys, chosen)
    return chosen.reshape(-1).astype(jnp.int32)


def with_ends(drawn, key, low, top_value):
    longest = drawn.shape.index(max(drawn.shape))
    spots = []
    for shift in (0, 1):
        where = [jax.random.randint(jax.random.fold_in(key, axis), (), 0, length) for axis, length in enumerate(drawn.shape)]
        where[longest] = (where[longest] + shift) % drawn.shape[longest]
        spots.append(tuple(where))
    return drawn.at[spots[0]].set(low).at[spots[1]].set(top_value)


def setup_inputs(seed: int = 0) -> dict:
    streams_of = jax.random.split(jax.random.key(seed), 5)
    return {
        "columns": draw_columns(jax.random.fold_in(streams_of[4], 71), 0),
        "counts": with_ends(jax.random.randint(streams_of[1], (CELLS, NNZ_MAX), 1, 64), jax.random.fold_in(streams_of[1], 1), 1, 63).astype(jnp.int32),
        "nnz_count": draw_nnz_count(jax.random.fold_in(streams_of[4], 71), 0),
        "selected": draw_selected(jax.random.fold_in(streams_of[4], 71), 0),
    }


target_sum = 10000.0
var_floor = 0.01
clip_value = 10.0

def reference(columns, counts, nnz_count, selected):
    slot = lax.broadcasted_iota(jnp.int32, counts.shape, 1)
    live = slot < nnz_count[:, None]
    raw = jnp.where(live, counts.astype(jnp.float32), jnp.float32(0.0))
    library = lax.optimization_barrier(jnp.sum(raw, axis=1, keepdims=True))
    values = jnp.log1p(raw * (target_sum / library))
    genes = jnp.where(live, columns, 0).astype(jnp.int32).reshape(-1)
    flat = values.reshape(-1)
    total = jax.ops.segment_sum(flat, genes, num_segments=GENES)
    square = jax.ops.segment_sum(flat * flat, genes, num_segments=GENES)
    mean = total / CELLS
    variance = square / CELLS - mean * mean
    gene_stats = jnp.stack([mean, variance])
    table = jnp.full((GENES,), SEL, jnp.int32).at[selected].set(jnp.arange(SEL, dtype=jnp.int32))
    position = table[genes]
    rows = jnp.repeat(jnp.arange(CELLS, dtype=jnp.int32), NNZ_MAX)
    index = rows * (SEL + 1) + position
    dense = jax.ops.segment_sum(flat, index, num_segments=CELLS * (SEL + 1)).reshape(CELLS, SEL + 1)[:, :SEL]
    mean_sel = mean[selected]
    scale_sel = jnp.sqrt(jnp.maximum(variance[selected], var_floor))
    pca_input = jnp.clip((dense - mean_sel[None, :]) / scale_sel[None, :], -clip_value, clip_value).astype(jnp.bfloat16)
    return (gene_stats, pca_input)
```

```python
import functools

import jax
import jax.numpy as jnp
from jax import lax
from jax.experimental import pallas as pl
from jax.experimental.pallas import tpu as pltpu
from jax.sharding import PartitionSpec as P

GENES = 32768
BLOCK = 16
LANES = 128

target_sum = 10000.0
var_floor = 0.01
clip_value = 10.0

MESH = pl.DeviceIdType.MESH


def local_kernel(
    owners, columns_ref, counts_ref, nnz_ref, selected_ref, sums_ref, sel_sums_ref, dense_ref,
    value_rows, high_rows, low_rows, offset_rows, block_values, block_offsets, table,
):
    cells, slots = columns_ref.shape
    high_count = GENES // (BLOCK * LANES)
    rows = high_count // owners
    bf16, f32 = jnp.bfloat16, jnp.float32

    sub = lax.broadcasted_iota(jnp.int32, (cells, cells), 0)
    lane = lax.broadcasted_iota(jnp.int32, (cells, cells), 1)
    live_count = jnp.sum(jnp.where(sub == lane, nnz_ref[...], 0), axis=1, keepdims=True)
    slot = lax.broadcasted_iota(jnp.int32, (cells, slots), 1)
    live = slot < live_count
    raw = jnp.where(live, counts_ref[...].astype(f32), 0.0)
    library = jnp.sum(raw, axis=1, keepdims=True)
    value_rows[...] = jnp.log1p(raw * (target_sum / library))
    genes = columns_ref[...]
    high_rows[...] = lax.shift_right_logical(genes, 11).astype(f32)
    low_rows[...] = (lax.shift_right_logical(genes, 4) & (LANES - 1)).astype(f32)
    offset_rows[...] = jnp.where(live, genes & (BLOCK - 1), 0).astype(f32)

    ids = lax.broadcasted_iota(jnp.int32, (16, slots), 0).astype(f32).astype(bf16)

    def spread(ref, c):
        return jnp.broadcast_to(ref[pl.ds(c, 1), :], (16, slots)).astype(bf16)

    def one_cell(c, carry):
        zero, one = bf16(0.0), bf16(1.0)
        hit = spread(high_rows, c) == ids
        left = jnp.concatenate(
            [jnp.where(hit, spread(value_rows, c), zero), jnp.where(hit, spread(offset_rows, c), zero)], axis=0
        )
        low = spread(low_rows, c)
        right = jnp.concatenate(
            [jnp.where(low == ids + bf16(16 * k), one, zero) for k in range(LANES // 16)], axis=0
        )
        placed = lax.dot_general(left, right, (((1,), (1,)), ((), ())), preferred_element_type=f32)
        block_values[c] = placed[:high_count]
        block_offsets[c] = placed[high_count:]
        return carry

    lax.fori_loop(0, cells, one_cell, 0, unroll=2)

    for half in range(high_count // 8):
        span = slice(8 * half, 8 * half + 8)

        def add_cell(c, carry):
            v = block_values[c, span, :]
            o = block_offsets[c, span, :]
            w = v * v
            out = []
            for k in range(BLOCK):
                hit = o == float(k)
                out.append(carry[2 * k] + jnp.where(hit, v, 0.0))
                out.append(carry[2 * k + 1] + jnp.where(hit, w, 0.0))
            return tuple(out)

        parts = lax.fori_loop(0, cells, add_cell, (jnp.zeros((8, LANES), f32),) * (2 * BLOCK))
        for k in range(BLOCK):
            for stat in range(2):
                part = parts[2 * k + stat]
                step = min(rows, 8)
                for first in range(0, 8, step):
                    row = 8 * half + first
                    owner, inner = row // rows, row % rows
                    sums_ref[k * owners + owner, pl.ds(stat * rows + inner, step), :] = part[first:first + step]

    for high in range(high_count):
        cols = slice(high * LANES, (high + 1) * LANES)
        table[0:cells, cols] = block_values[:, high, :].astype(bf16)
        table[cells:, cols] = block_offsets[:, high, :].astype(bf16)

    share = dense_ref.shape[2]
    tiles = share // LANES
    chunk = min(256, share)
    blocks = GENES // BLOCK
    sel_sums_ref[...] = jnp.zeros_like(sel_sums_ref)
    chunk_ids = lax.broadcasted_iota(jnp.int32, (16, chunk), 0).astype(f32).astype(bf16)
    for first in range(0, owners * share, chunk):
        picked = selected_ref[:, first:first + chunk]
        block = lax.shift_right_logical(picked, 4)
        pieces = []
        for group in range(blocks // 256):
            inside = jnp.where(lax.shift_right_logical(block, 8) == group, block & 255, -1).astype(f32)
            inside = jnp.broadcast_to(inside, (16, chunk)).astype(bf16)
            for k in range(16):
                pieces.append(jnp.where(inside == chunk_ids + bf16(16 * k), bf16(1.0), bf16(0.0)))
        found = jnp.dot(table[...], jnp.concatenate(pieces, axis=0), preferred_element_type=f32)
        wanted = (picked & (BLOCK - 1)).astype(f32)
        x = jnp.where(found[cells:] == wanted, found[:cells], 0.0)
        owner, start = first // share, first % share
        dense_ref[owner, :, start:start + chunk] = x.astype(bf16)
        total = jnp.sum(x, axis=0, keepdims=True)
        square = jnp.sum(x * x, axis=0, keepdims=True)
        for stat, line in enumerate((total, square)):
            for tile in range(chunk // LANES):
                r = stat * tiles + start // LANES + tile
                sel_sums_ref[r * owners + owner] = line[:, tile * LANES:(tile + 1) * LANES]


def exchange_kernel(
    sizes, cells, sums_ref, sel_sums_ref, dense_ref, stats_ref, sel_stats_ref, moved_ref,
    got, sel_got, mine, sel_mine, send_sem, recv_sem,
):
    nx, ny, nz = sizes
    teams = nx * ny
    n = teams * nz
    gx, gy, z = lax.axis_index("gx"), lax.axis_index("gy"), lax.axis_index("gz")
    r = gx * ny + gy
    me = r * nz + z

    def place(team, owner):
        return {"gx": lax.div(team, ny), "gy": lax.rem(team, ny), "gz": owner}

    def split(k):
        other = lax.rem(me + k, n)
        return other, place(lax.div(other, nz), lax.rem(other, nz))

    barrier = pltpu.get_barrier_semaphore()

    def greet(k, carry):
        pl.semaphore_signal(barrier, inc=1, device_id=split(k)[1], device_id_type=MESH)
        return carry

    lax.fori_loop(1, n, greet, 0)
    pl.semaphore_wait(barrier, n - 1)

    def send(src, dst, kind, where):
        pltpu.make_async_remote_copy(
            src_ref=src, dst_ref=dst, send_sem=send_sem.at[kind], recv_sem=recv_sem.at[kind],
            device_id=where, device_id_type=MESH,
        ).start()

    def scatter(k, carry):
        other, where = split(k)
        send(sums_ref.at[other], got.at[me], 0, where)
        send(sel_sums_ref.at[other], sel_got.at[me], 1, where)
        return carry

    lax.fori_loop(1, n, scatter, 0)

    def move(k, carry):
        owner = lax.rem(z + k, nz)
        send(dense_ref.at[owner], moved_ref.at[z], 2, place(r, owner))
        return carry

    lax.fori_loop(1, nz, move, 0)

    got[me] = sums_ref[me]
    sel_got[me] = sel_sums_ref[me]
    moved_ref[z] = dense_ref[z]

    def finish(sem, ref, count):
        span = ref.at[pl.ds(0, count)]
        pltpu.make_async_copy(span, span, sem).wait()

    finish(recv_sem.at[0], got, n - 1)
    finish(recv_sem.at[1], sel_got, n - 1)
    rows = mine.shape[0] // 2
    sums = jnp.sum(got[...], axis=0)
    mean = sums[:rows] * (1.0 / cells)
    mine[...] = jnp.concatenate([mean, sums[rows:] * (1.0 / cells) - mean * mean], axis=0)
    sel_mine[...] = jnp.sum(sel_got[...], axis=0)

    def gather(k, carry):
        where = place(lax.rem(r + k, teams), z)
        send(mine, stats_ref.at[r], 3, where)
        send(sel_mine, sel_stats_ref.at[r], 4, where)
        return carry

    lax.fori_loop(1, teams, gather, 0)
    stats_ref[r] = mine[...]
    sel_stats_ref[r] = sel_mine[...]
    finish(recv_sem.at[3], stats_ref, teams - 1)
    finish(recv_sem.at[4], sel_stats_ref, teams - 1)
    finish(recv_sem.at[2], moved_ref, nz - 1)
    finish(send_sem.at[0], got, n - 1)
    finish(send_sem.at[1], sel_got, n - 1)
    finish(send_sem.at[2], moved_ref, nz - 1)
    finish(send_sem.at[3], stats_ref, teams - 1)
    finish(send_sem.at[4], sel_stats_ref, teams - 1)


def final_kernel(cells, stats_ref, sel_stats_ref, moved_ref, gene_ref, pca_ref, turned):
    teams, double, lanes = stats_ref.shape
    rows = double // 2
    for stat in range(2):
        for row in range(rows):
            turned[row * lanes:(row + 1) * lanes, :] = jnp.transpose(stats_ref[:, stat * rows + row, :])
        lines = rows * lanes // 8
        parts = [turned[pl.ds(k, lines, stride=8), :] for k in range(8)]
        gene_ref[:, stat, :] = jnp.concatenate(parts, axis=1)
    owners, local, share = moved_ref.shape
    tiles = share // lanes
    for tile in range(tiles):
        mean = sel_stats_ref[tile] * (1.0 / cells)
        variance = sel_stats_ref[tiles + tile] * (1.0 / cells) - mean * mean
        scale = jnp.sqrt(jnp.maximum(variance, var_floor))
        cols = slice(tile * lanes, (tile + 1) * lanes)
        for owner in range(owners):
            x = moved_ref[owner, :, cols].astype(jnp.float32)
            y = jnp.clip((x - mean) / scale, -clip_value, clip_value)
            pca_ref[owner * local:(owner + 1) * local, cols] = y.astype(jnp.bfloat16)


def per_device(sizes, columns, counts, nnz_count, selected):
    f32, bf16 = jnp.float32, jnp.bfloat16
    nx, ny, owners = sizes
    teams = nx * ny
    n = teams * owners
    local, slots = columns.shape
    cells = local * n
    high_count = GENES // (BLOCK * LANES)
    rows = high_count // owners
    share = selected.shape[0] // owners
    assert teams == BLOCK and rows * owners == high_count and 2 * share // LANES <= teams
    vmem = pl.BlockSpec(memory_space=pltpu.VMEM)
    sums, sel_sums, dense = pl.pallas_call(
        functools.partial(local_kernel, owners),
        name="local_sums",
        out_shape=(
            jax.ShapeDtypeStruct((n, 2 * rows, LANES), f32),
            jax.ShapeDtypeStruct((n, 1, LANES), f32),
            jax.ShapeDtypeStruct((owners, local, share), bf16),
        ),
        in_specs=[vmem] * 4,
        out_specs=(vmem,) * 3,
        scratch_shapes=[pltpu.VMEM((local, slots), f32)] * 4
        + [pltpu.VMEM((local, high_count, LANES), f32)] * 2
        + [pltpu.VMEM((2 * local, GENES // BLOCK), bf16)],
    )(columns, counts, nnz_count.reshape(1, local), selected.reshape(1, -1))
    stats, sel_stats, moved = pl.pallas_call(
        functools.partial(exchange_kernel, sizes, cells),
        name="exchange",
        out_shape=(
            jax.ShapeDtypeStruct((teams, 2 * rows, LANES), f32),
            jax.ShapeDtypeStruct((teams, 1, LANES), f32),
            jax.ShapeDtypeStruct((owners, local, share), bf16),
        ),
        in_specs=[vmem] * 3,
        out_specs=(vmem,) * 3,
        scratch_shapes=[
            pltpu.VMEM((n, 2 * rows, LANES), f32),
            pltpu.VMEM((n, 1, LANES), f32),
            pltpu.VMEM((2 * rows, LANES), f32),
            pltpu.VMEM((1, LANES), f32),
            pltpu.SemaphoreType.DMA((5,)),
            pltpu.SemaphoreType.DMA((5,)),
        ],
        compiler_params=pltpu.CompilerParams(collective_id=0, has_side_effects=True),
    )(sums, sel_sums, dense)
    lines = GENES // owners // LANES
    gene_stats, pca_input = pl.pallas_call(
        functools.partial(final_kernel, cells),
        name="standardize",
        out_shape=(
            jax.ShapeDtypeStruct((lines, 2, LANES), f32),
            jax.ShapeDtypeStruct((owners * local, share), bf16),
        ),
        in_specs=[vmem] * 3,
        out_specs=(vmem,) * 2,
        scratch_shapes=[pltpu.VMEM((rows * LANES, teams), f32)],
    )(stats, sel_stats, moved)
    return (gene_stats.transpose(1, 0, 2).reshape(2, -1), pca_input)


def solution(mesh):
    sizes = tuple(mesh.shape[axis] for axis in ("gx", "gy", "gz"))
    return jax.shard_map(
        functools.partial(per_device, sizes),
        mesh=mesh,
        in_specs=(
            P(("gx", "gy", "gz"), None),
            P(("gx", "gy", "gz"), None),
            P(("gx", "gy", "gz")),
            P(),
        ),
        out_specs=(P(None, "gz"), P(("gx", "gy"), "gz")),
        check_vma=False,
    )
```

```python
import functools

import jax
import jax.numpy as jnp
from jax import lax
from jax.experimental import pallas as pl
from jax.experimental.pallas import tpu as pltpu
from jax.sharding import PartitionSpec as P

GENES = 32768
BLOCK = 16
LANES = 128

target_sum = 10000.0
var_floor = 0.01
clip_value = 10.0

MESH = pl.DeviceIdType.MESH


def fused_kernel(
    sizes, cells, columns_ref, counts_ref, nnz_ref, selected_ref, stats_ref, sel_stats_ref, moved_ref,
    value_rows, high_rows, low_rows, offset_rows, block_values, block_offsets, table,
    sums_ref, sel_sums_ref, dense_ref, got, sel_got, mine, sel_mine, send_sem, recv_sem,
):
    nx, ny, owners = sizes
    teams = nx * ny
    n = teams * owners
    gx, gy, z = lax.axis_index("gx"), lax.axis_index("gy"), lax.axis_index("gz")
    r = gx * ny + gy
    me = r * owners + z

    def place(team, owner):
        return {"gx": lax.div(team, ny), "gy": lax.rem(team, ny), "gz": owner}

    def split(k):
        other = lax.rem(me + k, n)
        return other, place(lax.div(other, owners), lax.rem(other, owners))

    barrier = pltpu.get_barrier_semaphore()

    def greet(k, carry):
        pl.semaphore_signal(barrier, inc=1, device_id=split(k)[1], device_id_type=MESH)
        return carry

    lax.fori_loop(1, n, greet, 0)

    def send(src, dst, kind, where):
        pltpu.make_async_remote_copy(
            src_ref=src, dst_ref=dst, send_sem=send_sem.at[kind], recv_sem=recv_sem.at[kind],
            device_id=where, device_id_type=MESH,
        ).start()

    def finish(sem, ref, count):
        span = ref.at[pl.ds(0, count)]
        pltpu.make_async_copy(span, span, sem).wait()

    local, slots = columns_ref.shape
    high_count = GENES // (BLOCK * LANES)
    rows = high_count // owners
    bf16, f32 = jnp.bfloat16, jnp.float32

    sub = lax.broadcasted_iota(jnp.int32, (local, local), 0)
    lane = lax.broadcasted_iota(jnp.int32, (local, local), 1)
    live_count = jnp.sum(jnp.where(sub == lane, nnz_ref[...], 0), axis=1, keepdims=True)
    slot = lax.broadcasted_iota(jnp.int32, (local, slots), 1)
    live = slot < live_count
    raw = jnp.where(live, counts_ref[...].astype(f32), 0.0)
    library = jnp.sum(raw, axis=1, keepdims=True)
    value_rows[...] = jnp.log1p(raw * (target_sum / library))
    genes = columns_ref[...]
    high_rows[...] = lax.shift_right_logical(genes, 11).astype(f32)
    low_rows[...] = (lax.shift_right_logical(genes, 4) & (LANES - 1)).astype(f32)
    offset_rows[...] = jnp.where(live, genes & (BLOCK - 1), 0).astype(f32)

    ids = lax.broadcasted_iota(jnp.int32, (16, slots), 0).astype(f32).astype(bf16)

    def spread(ref, c):
        return jnp.broadcast_to(ref[pl.ds(c, 1), :], (16, slots)).astype(bf16)

    def one_cell(c, carry):
        zero, one = bf16(0.0), bf16(1.0)
        hit = spread(high_rows, c) == ids
        left = jnp.concatenate(
            [jnp.where(hit, spread(value_rows, c), zero), jnp.where(hit, spread(offset_rows, c), zero)], axis=0
        )
        low = spread(low_rows, c)
        right = jnp.concatenate(
            [jnp.where(low == ids + bf16(16 * k), one, zero) for k in range(LANES // 16)], axis=0
        )
        placed = lax.dot_general(left, right, (((1,), (1,)), ((), ())), preferred_element_type=f32)
        block_values[c] = placed[:high_count]
        block_offsets[c] = placed[high_count:]
        return carry

    lax.fori_loop(0, local, one_cell, 0, unroll=2)

    for half in range(high_count // 8):
        span = slice(8 * half, 8 * half + 8)

        def add_cell(c, carry):
            v = block_values[c, span, :]
            o = block_offsets[c, span, :]
            w = v * v
            out = []
            for k in range(BLOCK):
                hit = o == float(k)
                out.append(carry[2 * k] + jnp.where(hit, v, 0.0))
                out.append(carry[2 * k + 1] + jnp.where(hit, w, 0.0))
            return tuple(out)

        parts = lax.fori_loop(0, local, add_cell, (jnp.zeros((8, LANES), f32),) * (2 * BLOCK))
        for k in range(BLOCK):
            for stat in range(2):
                part = parts[2 * k + stat]
                step = min(rows, 8)
                for first in range(0, 8, step):
                    row = 8 * half + first
                    owner, inner = row // rows, row % rows
                    sums_ref[k * owners + owner, pl.ds(stat * rows + inner, step), :] = part[first:first + step]

    for high in range(high_count):
        cols = slice(high * LANES, (high + 1) * LANES)
        table[0:local, cols] = block_values[:, high, :].astype(bf16)
        table[local:, cols] = block_offsets[:, high, :].astype(bf16)

    pl.semaphore_wait(barrier, n - 1)

    def scatter(k, carry):
        other, where = split(k)
        send(sums_ref.at[other], got.at[me], 0, where)
        return carry

    lax.fori_loop(1, n, scatter, 0)
    got[me] = sums_ref[me]

    share = dense_ref.shape[2]
    tiles = share // LANES
    chunk = min(256, share)
    blocks = GENES // BLOCK
    sel_sums_ref[...] = jnp.zeros_like(sel_sums_ref)
    chunk_ids = lax.broadcasted_iota(jnp.int32, (16, chunk), 0).astype(f32).astype(bf16)
    for first in range(0, owners * share, chunk):
        picked = selected_ref[:, first:first + chunk]
        block = lax.shift_right_logical(picked, 4)
        pieces = []
        for group in range(blocks // 256):
            inside = jnp.where(lax.shift_right_logical(block, 8) == group, block & 255, -1).astype(f32)
            inside = jnp.broadcast_to(inside, (16, chunk)).astype(bf16)
            for k in range(16):
                pieces.append(jnp.where(inside == chunk_ids + bf16(16 * k), bf16(1.0), bf16(0.0)))
        found = jnp.dot(table[...], jnp.concatenate(pieces, axis=0), preferred_element_type=f32)
        wanted = (picked & (BLOCK - 1)).astype(f32)
        x = jnp.where(found[local:] == wanted, found[:local], 0.0)
        owner, start = first // share, first % share
        dense_ref[owner, :, start:start + chunk] = x.astype(bf16)
        total = jnp.sum(x, axis=0, keepdims=True)
        square = jnp.sum(x * x, axis=0, keepdims=True)
        for stat, line in enumerate((total, square)):
            for tile in range(chunk // LANES):
                line_row = stat * tiles + start // LANES + tile
                sel_sums_ref[line_row * owners + owner] = line[:, tile * LANES:(tile + 1) * LANES]

    def move(k, carry):
        owner = lax.rem(z + k, owners)
        send(dense_ref.at[owner], moved_ref.at[z], 2, place(r, owner))
        return carry

    def sel_scatter(k, carry):
        other, where = split(k)
        send(sel_sums_ref.at[other], sel_got.at[me], 1, where)
        return carry

    lax.fori_loop(1, n, sel_scatter, 0)
    lax.fori_loop(1, owners, move, 0)
    sel_got[me] = sel_sums_ref[me]
    moved_ref[z] = dense_ref[z]

    finish(recv_sem.at[0], got, n - 1)
    sums = jnp.sum(got[...], axis=0)
    mean = sums[:rows] * (1.0 / cells)
    mine[...] = jnp.concatenate([mean, sums[rows:] * (1.0 / cells) - mean * mean], axis=0)

    def gather(k, carry):
        send(mine, stats_ref.at[r], 3, place(lax.rem(r + k, teams), z))
        return carry

    def sel_gather(k, carry):
        send(sel_mine, sel_stats_ref.at[r], 4, place(lax.rem(r + k, teams), z))
        return carry

    lax.fori_loop(1, teams, gather, 0)
    finish(recv_sem.at[1], sel_got, n - 1)
    sel_mine[...] = jnp.sum(sel_got[...], axis=0)
    stats_ref[r] = mine[...]
    lax.fori_loop(1, teams, sel_gather, 0)
    sel_stats_ref[r] = sel_mine[...]
    finish(recv_sem.at[2], moved_ref, owners - 1)
    finish(send_sem.at[0], got, n - 1)
    finish(send_sem.at[1], sel_got, n - 1)
    finish(send_sem.at[2], moved_ref, owners - 1)
    finish(recv_sem.at[3], stats_ref, teams - 1)
    finish(recv_sem.at[4], sel_stats_ref, teams - 1)
    finish(send_sem.at[3], stats_ref, teams - 1)
    finish(send_sem.at[4], sel_stats_ref, teams - 1)


def final_kernel(cells, stats_ref, sel_stats_ref, moved_ref, gene_ref, pca_ref, turned):
    teams, double, lanes = stats_ref.shape
    rows = double // 2
    for stat in range(2):
        for row in range(rows):
            turned[row * lanes:(row + 1) * lanes, :] = jnp.transpose(stats_ref[:, stat * rows + row, :])
        lines = rows * lanes // 8
        parts = [turned[pl.ds(k, lines, stride=8), :] for k in range(8)]
        gene_ref[:, stat, :] = jnp.concatenate(parts, axis=1)
    owners, local, share = moved_ref.shape
    tiles = share // lanes
    for tile in range(tiles):
        mean = sel_stats_ref[tile] * (1.0 / cells)
        variance = sel_stats_ref[tiles + tile] * (1.0 / cells) - mean * mean
        scale = jnp.sqrt(jnp.maximum(variance, var_floor))
        cols = slice(tile * lanes, (tile + 1) * lanes)
        for owner in range(owners):
            x = moved_ref[owner, :, cols].astype(jnp.float32)
            y = jnp.clip((x - mean) / scale, -clip_value, clip_value)
            pca_ref[owner * local:(owner + 1) * local, cols] = y.astype(jnp.bfloat16)


def per_device(sizes, columns, counts, nnz_count, selected):
    f32, bf16 = jnp.float32, jnp.bfloat16
    nx, ny, owners = sizes
    teams = nx * ny
    n = teams * owners
    local, slots = columns.shape
    cells = local * n
    high_count = GENES // (BLOCK * LANES)
    rows = high_count // owners
    share = selected.shape[0] // owners
    assert teams == BLOCK and rows * owners == high_count and 2 * share // LANES <= teams
    vmem = pl.BlockSpec(memory_space=pltpu.VMEM)
    stats, sel_stats, moved = pl.pallas_call(
        functools.partial(fused_kernel, sizes, cells),
        name="sums_and_exchange",
        out_shape=(
            jax.ShapeDtypeStruct((teams, 2 * rows, LANES), f32),
            jax.ShapeDtypeStruct((teams, 1, LANES), f32),
            jax.ShapeDtypeStruct((owners, local, share), bf16),
        ),
        in_specs=[vmem] * 4,
        out_specs=(vmem,) * 3,
        scratch_shapes=[pltpu.VMEM((local, slots), f32)] * 4
        + [pltpu.VMEM((local, high_count, LANES), f32)] * 2
        + [pltpu.VMEM((2 * local, GENES // BLOCK), bf16)]
        + [
            pltpu.VMEM((n, 2 * rows, LANES), f32),
            pltpu.VMEM((n, 1, LANES), f32),
            pltpu.VMEM((owners, local, share), bf16),
            pltpu.VMEM((n, 2 * rows, LANES), f32),
            pltpu.VMEM((n, 1, LANES), f32),
            pltpu.VMEM((2 * rows, LANES), f32),
            pltpu.VMEM((1, LANES), f32),
            pltpu.SemaphoreType.DMA((5,)),
            pltpu.SemaphoreType.DMA((5,)),
        ],
        compiler_params=pltpu.CompilerParams(collective_id=0, has_side_effects=True),
    )(columns, counts, nnz_count.reshape(1, local), selected.reshape(1, -1))
    lines = GENES // owners // LANES
    gene_stats, pca_input = pl.pallas_call(
        functools.partial(final_kernel, cells),
        name="standardize",
        out_shape=(
            jax.ShapeDtypeStruct((lines, 2, LANES), f32),
            jax.ShapeDtypeStruct((owners * local, share), bf16),
        ),
        in_specs=[vmem] * 3,
        out_specs=(vmem,) * 2,
        scratch_shapes=[pltpu.VMEM((rows * LANES, teams), f32)],
    )(stats, sel_stats, moved)
    return (gene_stats.transpose(1, 0, 2).reshape(2, -1), pca_input)


def solution(mesh):
    sizes = tuple(mesh.shape[axis] for axis in ("gx", "gy", "gz"))
    return jax.shard_map(
        functools.partial(per_device, sizes),
        mesh=mesh,
        in_specs=(
            P(("gx", "gy", "gz"), None),
            P(("gx", "gy", "gz"), None),
            P(("gx", "gy", "gz")),
            P(),
        ),
        out_specs=(P(None, "gz"), P(("gx", "gy"), "gz")),
        check_vma=False,
    )
```

```python
import functools

import jax
import jax.numpy as jnp
from jax import lax
from jax.experimental import pallas as pl
from jax.experimental.pallas import tpu as pltpu
from jax.sharding import PartitionSpec as P

GENES = 32768
BLOCK = 16
LANES = 128

target_sum = 10000.0
var_floor = 0.01
clip_value = 10.0

MESH = pl.DeviceIdType.MESH


def fused_kernel(
    sizes, cells, columns_ref, counts_ref, nnz_ref, selected_ref, stats_ref, sel_stats_ref, moved_ref,
    value_rows, high_rows, low_rows, offset_rows, block_values, block_offsets, table,
    sums_ref, sel_sums_ref, dense_ref, got, sel_got, mine, sel_mine, send_sem, recv_sem,
):
    nx, ny, owners = sizes
    teams = nx * ny
    n = teams * owners
    gx, gy, z = lax.axis_index("gx"), lax.axis_index("gy"), lax.axis_index("gz")
    r = gx * ny + gy
    me = r * owners + z

    def place(team, owner):
        return {"gx": lax.div(team, ny), "gy": lax.rem(team, ny), "gz": owner}

    def split(k):
        other = lax.rem(me + k, n)
        return other, place(lax.div(other, owners), lax.rem(other, owners))

    barrier = pltpu.get_barrier_semaphore()

    def greet(k, carry):
        pl.semaphore_signal(barrier, inc=1, device_id=split(k)[1], device_id_type=MESH)
        return carry

    lax.fori_loop(1, n, greet, 0)

    def send(src, dst, kind, where):
        pltpu.make_async_remote_copy(
            src_ref=src, dst_ref=dst, send_sem=send_sem.at[kind], recv_sem=recv_sem.at[kind],
            device_id=where, device_id_type=MESH,
        ).start()

    def finish(sem, ref, count):
        span = ref.at[pl.ds(0, count)]
        pltpu.make_async_copy(span, span, sem).wait()

    local, slots = columns_ref.shape
    high_count = GENES // (BLOCK * LANES)
    rows = high_count // owners
    bf16, f32 = jnp.bfloat16, jnp.float32

    sub = lax.broadcasted_iota(jnp.int32, (local, local), 0)
    lane = lax.broadcasted_iota(jnp.int32, (local, local), 1)
    live_count = jnp.sum(jnp.where(sub == lane, nnz_ref[...], 0), axis=1, keepdims=True)
    slot = lax.broadcasted_iota(jnp.int32, (local, slots), 1)
    live = slot < live_count
    raw = jnp.where(live, counts_ref[...].astype(f32), 0.0)
    library = jnp.sum(raw, axis=1, keepdims=True)
    value_rows[...] = jnp.log1p(raw * (target_sum / library))
    genes = columns_ref[...]
    upper = (lax.shift_right_logical(genes, 10) & 1) * high_count
    high_rows[...] = (lax.shift_right_logical(genes, 11) + upper).astype(f32)
    low_rows[...] = (lax.shift_right_logical(genes, 4) & (LANES // 2 - 1)).astype(f32)
    offset_rows[...] = jnp.where(live, genes & (BLOCK - 1), 0).astype(f32)

    ids = lax.broadcasted_iota(jnp.int32, (16, slots), 0).astype(f32).astype(bf16)

    def spread(ref, c):
        return jnp.broadcast_to(ref[pl.ds(c, 1), :], (16, slots)).astype(bf16)

    def one_cell(c, carry):
        zero, one = bf16(0.0), bf16(1.0)
        high = spread(high_rows, c)
        hits = [high == ids + bf16(high_count * k) for k in range(2)]
        value, offset = spread(value_rows, c), spread(offset_rows, c)
        left = jnp.concatenate(
            [jnp.where(hit, line, zero) for line in (value, offset) for hit in hits], axis=0
        )
        low = spread(low_rows, c)
        right = jnp.concatenate(
            [jnp.where(low == ids + bf16(16 * k), one, zero) for k in range(LANES // 32)], axis=0
        )
        placed = lax.dot_general(left, right, (((1,), (1,)), ((), ())), preferred_element_type=f32)
        quarters = [placed[high_count * k:high_count * (k + 1)] for k in range(4)]
        block_values[c] = jnp.concatenate(quarters[:2], axis=1)
        block_offsets[c] = jnp.concatenate(quarters[2:], axis=1)
        return carry

    lax.fori_loop(0, local, one_cell, 0, unroll=8)

    for half in range(high_count // 8):
        span = slice(8 * half, 8 * half + 8)

        def add_cell(c, carry):
            v = block_values[c, span, :]
            o = block_offsets[c, span, :]
            w = v * v
            out = []
            for k in range(BLOCK):
                hit = o == float(k)
                out.append(carry[2 * k] + jnp.where(hit, v, 0.0))
                out.append(carry[2 * k + 1] + jnp.where(hit, w, 0.0))
            return tuple(out)

        parts = lax.fori_loop(0, local, add_cell, (jnp.zeros((8, LANES), f32),) * (2 * BLOCK))
        for k in range(BLOCK):
            near = parts[2 * k] * (1.0 / local)
            spare = parts[2 * k + 1] - parts[2 * k] * near
            step = min(rows, 8)
            for first in range(0, 8, step):
                owner = (8 * half + first) // rows
                pair = jnp.concatenate([near[first:first + step], spare[first:first + step]], axis=0)
                sums_ref[k * owners + owner] = pair.astype(bf16)

    for high in range(high_count):
        cols = slice(high * LANES, (high + 1) * LANES)
        table[0:local, cols] = block_values[:, high, :].astype(bf16)
        table[local:, cols] = block_offsets[:, high, :].astype(bf16)

    pl.semaphore_wait(barrier, n - 1)

    def scatter(k, carry):
        other, where = split(k)
        send(sums_ref.at[other], got.at[me], 0, where)
        return carry

    lax.fori_loop(1, n, scatter, 0)
    got[me] = sums_ref[me]

    share = dense_ref.shape[2]
    tiles = share // LANES
    chunk = min(256, share)
    blocks = GENES // BLOCK
    sel_sums_ref[...] = jnp.zeros_like(sel_sums_ref)
    chunk_ids = lax.broadcasted_iota(jnp.int32, (16, chunk), 0).astype(f32).astype(bf16)
    for first in range(0, owners * share, chunk):
        picked = selected_ref[:, first:first + chunk]
        block = lax.shift_right_logical(picked, 4)
        pieces = []
        for group in range(blocks // 256):
            inside = jnp.where(lax.shift_right_logical(block, 8) == group, block & 255, -1).astype(f32)
            inside = jnp.broadcast_to(inside, (16, chunk)).astype(bf16)
            for k in range(16):
                pieces.append(jnp.where(inside == chunk_ids + bf16(16 * k), bf16(1.0), bf16(0.0)))
        found = jnp.dot(table[...], jnp.concatenate(pieces, axis=0), preferred_element_type=f32)
        wanted = (picked & (BLOCK - 1)).astype(f32)
        x = jnp.where(found[local:] == wanted, found[:local], 0.0)
        owner, start = first // share, first % share
        dense_ref[owner, :, start:start + chunk] = x.astype(bf16)
        total = jnp.sum(x, axis=0, keepdims=True)
        square = jnp.sum(x * x, axis=0, keepdims=True)
        for stat, line in enumerate((total, square)):
            for tile in range(chunk // LANES):
                line_row = stat * tiles + start // LANES + tile
                sel_sums_ref[line_row * owners + owner] = line[:, tile * LANES:(tile + 1) * LANES]

    def move(k, carry):
        owner = lax.rem(z + k, owners)
        send(dense_ref.at[owner], moved_ref.at[z], 2, place(r, owner))
        return carry

    def sel_scatter(k, carry):
        other, where = split(k)
        send(sel_sums_ref.at[other], sel_got.at[me], 1, where)
        return carry

    lax.fori_loop(1, n, sel_scatter, 0)
    lax.fori_loop(1, owners, move, 0)
    sel_got[me] = sel_sums_ref[me]
    moved_ref[z] = dense_ref[z]

    finish(recv_sem.at[0], got, n - 1)
    parts = got[...].astype(f32)
    means = parts[:, :rows]
    mean = jnp.sum(means, axis=0) * (1.0 / n)
    away = means - mean[None]
    variance = jnp.sum(parts[:, rows:] + (away * away) * float(local), axis=0) * (1.0 / cells)
    mine[...] = jnp.concatenate([mean, variance], axis=0).astype(bf16)

    def gather(k, carry):
        send(mine, stats_ref.at[r], 3, place(lax.rem(r + k, teams), z))
        return carry

    def sel_gather(k, carry):
        send(sel_mine, sel_stats_ref.at[r], 4, place(lax.rem(r + k, teams), z))
        return carry

    lax.fori_loop(1, teams, gather, 0)
    finish(recv_sem.at[1], sel_got, n - 1)
    sel_mine[...] = jnp.sum(sel_got[...], axis=0)
    stats_ref[r] = mine[...]
    lax.fori_loop(1, teams, sel_gather, 0)
    sel_stats_ref[r] = sel_mine[...]
    finish(recv_sem.at[2], moved_ref, owners - 1)
    finish(send_sem.at[0], got, n - 1)
    finish(send_sem.at[1], sel_got, n - 1)
    finish(send_sem.at[2], moved_ref, owners - 1)
    finish(recv_sem.at[3], stats_ref, teams - 1)
    finish(recv_sem.at[4], sel_stats_ref, teams - 1)
    finish(send_sem.at[3], stats_ref, teams - 1)
    finish(send_sem.at[4], sel_stats_ref, teams - 1)


def final_kernel(cells, stats_ref, sel_stats_ref, moved_ref, gene_ref, pca_ref, turned):
    teams, double, lanes = stats_ref.shape
    rows = double // 2
    stats = stats_ref[...].astype(jnp.float32)
    for stat in range(2):
        for row in range(rows):
            turned[row * lanes:(row + 1) * lanes, :] = jnp.transpose(stats[:, stat * rows + row, :])
        lines = rows * lanes // 8
        parts = [turned[pl.ds(k, lines, stride=8), :] for k in range(8)]
        gene_ref[:, stat, :] = jnp.concatenate(parts, axis=1)
    owners, local, share = moved_ref.shape
    tiles = share // lanes
    for tile in range(tiles):
        mean = sel_stats_ref[tile] * (1.0 / cells)
        variance = sel_stats_ref[tiles + tile] * (1.0 / cells) - mean * mean
        scale = jnp.sqrt(jnp.maximum(variance, var_floor))
        cols = slice(tile * lanes, (tile + 1) * lanes)
        for owner in range(owners):
            x = moved_ref[owner, :, cols].astype(jnp.float32)
            y = jnp.clip((x - mean) / scale, -clip_value, clip_value)
            pca_ref[owner * local:(owner + 1) * local, cols] = y.astype(jnp.bfloat16)


def per_device(sizes, columns, counts, nnz_count, selected):
    f32, bf16 = jnp.float32, jnp.bfloat16
    nx, ny, owners = sizes
    teams = nx * ny
    n = teams * owners
    local, slots = columns.shape
    cells = local * n
    high_count = GENES // (BLOCK * LANES)
    rows = high_count // owners
    share = selected.shape[0] // owners
    assert teams == BLOCK and rows * owners == high_count and rows <= 8 and 2 * share // LANES <= teams
    vmem = pl.BlockSpec(memory_space=pltpu.VMEM)
    stats, sel_stats, moved = pl.pallas_call(
        functools.partial(fused_kernel, sizes, cells),
        name="sums_and_exchange",
        out_shape=(
            jax.ShapeDtypeStruct((teams, 2 * rows, LANES), bf16),
            jax.ShapeDtypeStruct((teams, 1, LANES), f32),
            jax.ShapeDtypeStruct((owners, local, share), bf16),
        ),
        in_specs=[vmem] * 4,
        out_specs=(vmem,) * 3,
        scratch_shapes=[pltpu.VMEM((local, slots), f32)] * 4
        + [pltpu.VMEM((local, high_count, LANES), f32)] * 2
        + [pltpu.VMEM((2 * local, GENES // BLOCK), bf16)]
        + [
            pltpu.VMEM((n, 2 * rows, LANES), bf16),
            pltpu.VMEM((n, 1, LANES), f32),
            pltpu.VMEM((owners, local, share), bf16),
            pltpu.VMEM((n, 2 * rows, LANES), bf16),
            pltpu.VMEM((n, 1, LANES), f32),
            pltpu.VMEM((2 * rows, LANES), bf16),
            pltpu.VMEM((1, LANES), f32),
            pltpu.SemaphoreType.DMA((5,)),
            pltpu.SemaphoreType.DMA((5,)),
        ],
        compiler_params=pltpu.CompilerParams(collective_id=0, has_side_effects=True),
    )(columns, counts, nnz_count.reshape(1, local), selected.reshape(1, -1))
    lines = GENES // owners // LANES
    gene_stats, pca_input = pl.pallas_call(
        functools.partial(final_kernel, cells),
        name="standardize",
        out_shape=(
            jax.ShapeDtypeStruct((lines, 2, LANES), f32),
            jax.ShapeDtypeStruct((owners * local, share), bf16),
        ),
        in_specs=[vmem] * 3,
        out_specs=(vmem,) * 2,
        scratch_shapes=[pltpu.VMEM((rows * LANES, teams), f32)],
    )(stats, sel_stats, moved)
    return (gene_stats.transpose(1, 0, 2).reshape(2, -1), pca_input)


def solution(mesh):
    sizes = tuple(mesh.shape[axis] for axis in ("gx", "gy", "gz"))
    return jax.shard_map(
        functools.partial(per_device, sizes),
        mesh=mesh,
        in_specs=(
            P(("gx", "gy", "gz"), None),
            P(("gx", "gy", "gz"), None),
            P(("gx", "gy", "gz")),
            P(),
        ),
        out_specs=(P(None, "gz"), P(("gx", "gy"), "gz")),
        check_vma=False,
    )
```

```python
import functools

import jax
import jax.numpy as jnp
from jax import lax
from jax.experimental import pallas as pl
from jax.experimental.pallas import tpu as pltpu
from jax.sharding import PartitionSpec as P

GENES = 32768
BLOCK = 16
LANES = 128

target_sum = 10000.0
var_floor = 0.01
clip_value = 10.0

MESH = pl.DeviceIdType.MESH


def fused_kernel(
    sizes, cells, columns_ref, counts_ref, nnz_ref, selected_ref, stats_ref, sel_stats_ref, moved_ref,
    value_rows, high_rows, low_rows, offset_rows, block_values, block_offsets, table,
    sums_ref, sel_sums_ref, dense_ref, got, sel_got, mine, sel_mine, send_sem, recv_sem,
):
    nx, ny, owners = sizes
    teams = nx * ny
    n = teams * owners
    gx, gy, z = lax.axis_index("gx"), lax.axis_index("gy"), lax.axis_index("gz")
    r = gx * ny + gy
    me = r * owners + z

    def place(team, owner):
        return {"gx": lax.div(team, ny), "gy": lax.rem(team, ny), "gz": owner}

    def split(k):
        other = lax.rem(me + k, n)
        return other, place(lax.div(other, owners), lax.rem(other, owners))

    barrier = pltpu.get_barrier_semaphore()

    def greet(k, carry):
        pl.semaphore_signal(barrier, inc=1, device_id=split(k)[1], device_id_type=MESH)
        return carry

    lax.fori_loop(1, n, greet, 0)

    def send(src, dst, kind, where):
        pltpu.make_async_remote_copy(
            src_ref=src, dst_ref=dst, send_sem=send_sem.at[kind], recv_sem=recv_sem.at[kind],
            device_id=where, device_id_type=MESH,
        ).start()

    def finish(sem, ref, count):
        span = ref.at[pl.ds(0, count)]
        pltpu.make_async_copy(span, span, sem).wait()

    local, slots = columns_ref.shape
    high_count = GENES // (BLOCK * LANES)
    rows = high_count // owners
    bf16, f32 = jnp.bfloat16, jnp.float32

    sub = lax.broadcasted_iota(jnp.int32, (local, local), 0)
    lane = lax.broadcasted_iota(jnp.int32, (local, local), 1)
    live_count = jnp.sum(jnp.where(sub == lane, nnz_ref[...], 0), axis=1, keepdims=True)
    slot = lax.broadcasted_iota(jnp.int32, (local, slots), 1)
    live = slot < live_count
    raw = jnp.where(live, counts_ref[...].astype(f32), 0.0)
    library = jnp.sum(raw, axis=1, keepdims=True)
    value_rows[...] = jnp.log1p(raw * (target_sum / library))
    genes = columns_ref[...]
    upper = (lax.shift_right_logical(genes, 10) & 1) * high_count
    high_rows[...] = (lax.shift_right_logical(genes, 11) + upper).astype(f32)
    low_rows[...] = (lax.shift_right_logical(genes, 4) & (LANES // 2 - 1)).astype(f32)
    offset_rows[...] = jnp.where(live, genes & (BLOCK - 1), 0).astype(f32)

    ids = lax.broadcasted_iota(jnp.int32, (16, slots), 0).astype(f32).astype(bf16)

    def spread(ref, c):
        return jnp.broadcast_to(ref[pl.ds(c, 1), :], (16, slots)).astype(bf16)

    def one_cell(c, carry):
        zero, one = bf16(0.0), bf16(1.0)
        high = spread(high_rows, c)
        hits = [high == ids + bf16(high_count * k) for k in range(2)]
        value, offset = spread(value_rows, c), spread(offset_rows, c)
        left = jnp.concatenate(
            [jnp.where(hit, line, zero) for line in (value, offset) for hit in hits], axis=0
        )
        low = spread(low_rows, c)
        right = jnp.concatenate(
            [jnp.where(low == ids + bf16(16 * k), one, zero) for k in range(LANES // 32)], axis=0
        )
        placed = lax.dot_general(left, right, (((1,), (1,)), ((), ())), preferred_element_type=f32)
        quarters = [placed[high_count * k:high_count * (k + 1)] for k in range(4)]
        block_values[c] = jnp.concatenate(quarters[:2], axis=1)
        block_offsets[c] = jnp.concatenate(quarters[2:], axis=1)
        return carry

    lax.fori_loop(0, local, one_cell, 0, unroll=8)

    for half in range(high_count // 8):
        span = slice(8 * half, 8 * half + 8)

        def add_cell(c, carry):
            v = block_values[c, span, :]
            o = block_offsets[c, span, :]
            w = v * v
            out = []
            for k in range(BLOCK):
                hit = o == float(k)
                out.append(carry[2 * k] + jnp.where(hit, v, 0.0))
                out.append(carry[2 * k + 1] + jnp.where(hit, w, 0.0))
            return tuple(out)

        parts = lax.fori_loop(0, local, add_cell, (jnp.zeros((8, LANES), f32),) * (2 * BLOCK), unroll=4)
        for k in range(BLOCK):
            near = parts[2 * k] * (1.0 / local)
            spare = parts[2 * k + 1] - parts[2 * k] * near
            step = min(rows, 8)
            for first in range(0, 8, step):
                owner = (8 * half + first) // rows
                pair = jnp.concatenate([near[first:first + step], spare[first:first + step]], axis=0)
                sums_ref[k * owners + owner] = pair.astype(bf16)

    for high in range(high_count):
        cols = slice(high * LANES, (high + 1) * LANES)
        table[0:local, cols] = block_values[:, high, :].astype(bf16)
        table[local:, cols] = block_offsets[:, high, :].astype(bf16)

    pl.semaphore_wait(barrier, n - 1)

    def scatter(k, carry):
        other, where = split(k)
        send(sums_ref.at[other], got.at[me], 0, where)
        return carry

    lax.fori_loop(1, n, scatter, 0)
    got[me] = sums_ref[me]

    share = dense_ref.shape[2]
    tiles = share // LANES
    chunk = min(256, share)
    blocks = GENES // BLOCK
    sel_sums_ref[...] = jnp.zeros_like(sel_sums_ref)
    chunk_ids = lax.broadcasted_iota(jnp.int32, (16, chunk), 0).astype(f32).astype(bf16)
    for first in range(0, owners * share, chunk):
        picked = selected_ref[:, first:first + chunk]
        block = lax.shift_right_logical(picked, 4)
        pieces = []
        for group in range(blocks // 256):
            inside = jnp.where(lax.shift_right_logical(block, 8) == group, block & 255, -1).astype(f32)
            inside = jnp.broadcast_to(inside, (16, chunk)).astype(bf16)
            for k in range(16):
                pieces.append(jnp.where(inside == chunk_ids + bf16(16 * k), bf16(1.0), bf16(0.0)))
        found = jnp.dot(table[...], jnp.concatenate(pieces, axis=0), preferred_element_type=f32)
        wanted = (picked & (BLOCK - 1)).astype(f32)
        x = jnp.where(found[local:] == wanted, found[:local], 0.0)
        owner, start = first // share, first % share
        dense_ref[owner, :, start:start + chunk] = x.astype(bf16)
        total = jnp.sum(x, axis=0, keepdims=True)
        square = jnp.sum(x * x, axis=0, keepdims=True)
        for stat, line in enumerate((total, square)):
            for tile in range(chunk // LANES):
                line_row = stat * tiles + start // LANES + tile
                sel_sums_ref[line_row * owners + owner] = line[:, tile * LANES:(tile + 1) * LANES]

    def move(k, carry):
        owner = lax.rem(z + k, owners)
        send(dense_ref.at[owner], moved_ref.at[z], 2, place(r, owner))
        return carry

    def sel_scatter(k, carry):
        other, where = split(k)
        send(sel_sums_ref.at[other], sel_got.at[me], 1, where)
        return carry

    lax.fori_loop(1, n, sel_scatter, 0)
    lax.fori_loop(1, owners, move, 0)
    sel_got[me] = sel_sums_ref[me]
    moved_ref[z] = dense_ref[z]

    finish(recv_sem.at[0], got, n - 1)
    parts = got[...].astype(f32)
    means = parts[:, :rows]
    mean = jnp.sum(means, axis=0) * (1.0 / n)
    away = means - mean[None]
    variance = jnp.sum(parts[:, rows:] + (away * away) * float(local), axis=0) * (1.0 / cells)
    mine[...] = jnp.concatenate([mean, variance], axis=0).astype(bf16)

    def gather(k, carry):
        send(mine, stats_ref.at[r], 3, place(lax.rem(r + k, teams), z))
        return carry

    def sel_gather(k, carry):
        send(sel_mine, sel_stats_ref.at[r], 4, place(lax.rem(r + k, teams), z))
        return carry

    lax.fori_loop(1, teams, gather, 0)
    finish(recv_sem.at[1], sel_got, n - 1)
    sel_mine[...] = jnp.sum(sel_got[...], axis=0)
    stats_ref[r] = mine[...]
    lax.fori_loop(1, teams, sel_gather, 0)
    sel_stats_ref[r] = sel_mine[...]
    finish(recv_sem.at[2], moved_ref, owners - 1)
    finish(send_sem.at[0], got, n - 1)
    finish(send_sem.at[1], sel_got, n - 1)
    finish(send_sem.at[2], moved_ref, owners - 1)
    finish(recv_sem.at[3], stats_ref, teams - 1)
    finish(recv_sem.at[4], sel_stats_ref, teams - 1)
    finish(send_sem.at[3], stats_ref, teams - 1)
    finish(send_sem.at[4], sel_stats_ref, teams - 1)


def final_kernel(cells, stats_ref, sel_stats_ref, moved_ref, gene_ref, pca_ref, turned):
    teams, double, lanes = stats_ref.shape
    rows = double // 2
    stats = stats_ref[...].astype(jnp.float32)
    for stat in range(2):
        for row in range(rows):
            turned[row * lanes:(row + 1) * lanes, :] = jnp.transpose(stats[:, stat * rows + row, :])
        lines = rows * lanes // 8
        parts = [turned[pl.ds(k, lines, stride=8), :] for k in range(8)]
        gene_ref[:, stat, :] = jnp.concatenate(parts, axis=1)
    owners, local, share = moved_ref.shape
    tiles = share // lanes
    for tile in range(tiles):
        mean = sel_stats_ref[tile] * (1.0 / cells)
        variance = sel_stats_ref[tiles + tile] * (1.0 / cells) - mean * mean
        scale = jnp.sqrt(jnp.maximum(variance, var_floor))
        cols = slice(tile * lanes, (tile + 1) * lanes)
        for owner in range(owners):
            x = moved_ref[owner, :, cols].astype(jnp.float32)
            y = jnp.clip((x - mean) / scale, -clip_value, clip_value)
            pca_ref[owner * local:(owner + 1) * local, cols] = y.astype(jnp.bfloat16)


def per_device(sizes, columns, counts, nnz_count, selected):
    f32, bf16 = jnp.float32, jnp.bfloat16
    nx, ny, owners = sizes
    teams = nx * ny
    n = teams * owners
    local, slots = columns.shape
    cells = local * n
    high_count = GENES // (BLOCK * LANES)
    rows = high_count // owners
    share = selected.shape[0] // owners
    assert teams == BLOCK and rows * owners == high_count and rows <= 8 and 2 * share // LANES <= teams
    vmem = pl.BlockSpec(memory_space=pltpu.VMEM)
    stats, sel_stats, moved = pl.pallas_call(
        functools.partial(fused_kernel, sizes, cells),
        name="sums_and_exchange",
        out_shape=(
            jax.ShapeDtypeStruct((teams, 2 * rows, LANES), bf16),
            jax.ShapeDtypeStruct((teams, 1, LANES), f32),
            jax.ShapeDtypeStruct((owners, local, share), bf16),
        ),
        in_specs=[vmem] * 4,
        out_specs=(vmem,) * 3,
        scratch_shapes=[pltpu.VMEM((local, slots), f32)] * 4
        + [pltpu.VMEM((local, high_count, LANES), f32)] * 2
        + [pltpu.VMEM((2 * local, GENES // BLOCK), bf16)]
        + [
            pltpu.VMEM((n, 2 * rows, LANES), bf16),
            pltpu.VMEM((n, 1, LANES), f32),
            pltpu.VMEM((owners, local, share), bf16),
            pltpu.VMEM((n, 2 * rows, LANES), bf16),
            pltpu.VMEM((n, 1, LANES), f32),
            pltpu.VMEM((2 * rows, LANES), bf16),
            pltpu.VMEM((1, LANES), f32),
            pltpu.SemaphoreType.DMA((5,)),
            pltpu.SemaphoreType.DMA((5,)),
        ],
        compiler_params=pltpu.CompilerParams(collective_id=0, has_side_effects=True),
    )(columns, counts, nnz_count.reshape(1, local), selected.reshape(1, -1))
    lines = GENES // owners // LANES
    gene_stats, pca_input = pl.pallas_call(
        functools.partial(final_kernel, cells),
        name="standardize",
        out_shape=(
            jax.ShapeDtypeStruct((lines, 2, LANES), f32),
            jax.ShapeDtypeStruct((owners * local, share), bf16),
        ),
        in_specs=[vmem] * 3,
        out_specs=(vmem,) * 2,
        scratch_shapes=[pltpu.VMEM((rows * LANES, teams), f32)],
    )(stats, sel_stats, moved)
    return (gene_stats.transpose(1, 0, 2).reshape(2, -1), pca_input)


def solution(mesh):
    sizes = tuple(mesh.shape[axis] for axis in ("gx", "gy", "gz"))
    return jax.shard_map(
        functools.partial(per_device, sizes),
        mesh=mesh,
        in_specs=(
            P(("gx", "gy", "gz"), None),
            P(("gx", "gy", "gz"), None),
            P(("gx", "gy", "gz")),
            P(),
        ),
        out_specs=(P(None, "gz"), P(("gx", "gy"), "gz")),
        check_vma=False,
    )
```
